16 devices in a mesh: dep: 2 (over z), col: 2 (over y), row: 4 (over x, core).
Axes of the slice: x: 2, y: 2, z: 2, core: 2. Of those that a mesh axis runs over, the one named last changes fastest.
Arguments:
- a_mat: bfloat16 [12288, 12288], P('row', 'col')
- b_mat: bfloat16 [12288, 12288], P('row', 'col')
Outputs:
- output: float32 [12288, 12288], P('row', ('col', 'dep'))
All inputs are finite; a program needn't handle non-finite values.
Results may differ from the reference program's by a relative error of at most 0.001.
Values are sent between devices in bfloat16 or wider.
A program may use at most 1 GiB of HBM per device.

```python
import jax
import jax.numpy as jnp

N = 12288


def setup_inputs(seed: int = 0) -> dict:
    key = jax.random.key(seed)
    key_a, key_b = jax.random.split(key)
    a_mat = (jax.random.normal(key_a, (N, N), jnp.float32) * N ** -0.5).astype(jnp.bfloat16)
    b_mat = jax.random.normal(key_b, (N, N), jnp.float32).astype(jnp.bfloat16)
    return {"a_mat": a_mat, "b_mat": b_mat}


def reference(a_mat, b_mat):
    return jnp.dot(a_mat, b_mat, preferred_element_type=jnp.float32)
```

```python
import functools

import jax
import jax.numpy as jnp
from jax import lax
from jax.experimental import pallas as pl
from jax.experimental.pallas import tpu as pltpu
from jax.sharding import PartitionSpec as P

MESH = pl.DeviceIdType.MESH
KC = 128
Q = 3
YD = 4
ZD = 4
TILES = 6
XD = 2


def gather_kernel(
    a_ref, b_ref,
    c_ref, abuf, bbuf, ay, az, bx, bp, bq,
    ysend, yrecv, zsend, zrecv, xsend, xrecv, psend, precv, qsend, qrecv, ldsem,
):
    z, y, i = lax.axis_index("dep"), lax.axis_index("col"), lax.axis_index("row")
    m = a_ref.shape[0]
    mq, tn = m // Q, m // TILES
    rounds = m // KC
    ticks = rounds * Q
    z_to, y_to = {"dep": 1 - z}, {"col": 1 - y}
    x_to, p_to = {"row": lax.rem(i + 2, 4)}, {"row": i + 1 - 2 * lax.rem(i, 2)}

    def y_copy(s):
        t, rows = s // Q, pl.ds(pl.multiple_of(lax.rem(s, Q) * mq, mq), mq)
        cols = pl.ds(pl.multiple_of(z * m + t * KC, KC), KC)
        return pltpu.make_async_remote_copy(
            a_ref.at[rows, cols], ay.at[t, rows, :], ysend.at[lax.rem(s, YD)], yrecv.at[s],
            device_id=y_to, device_id_type=MESH,
        )

    def z_copy(s):
        t, rows = s // Q, pl.ds(pl.multiple_of(lax.rem(s, Q) * mq, mq), mq)
        return pltpu.make_async_remote_copy(
            ay.at[t, rows, :], az.at[t, rows, :], zsend.at[lax.rem(s, ZD)], zrecv.at[s],
            device_id=z_to, device_id_type=MESH,
        )

    def b_rows(t):
        return pl.ds(pl.multiple_of(t * KC, KC), KC)

    def b_piece(t):
        return b_ref.at[b_rows(t), pl.ds(pl.multiple_of(z * m, m), m)]

    def x_copy(t):
        return pltpu.make_async_remote_copy(
            b_piece(t), bx.at[b_rows(t), :], xsend.at[lax.rem(t, XD)], xrecv.at[t],
            device_id=x_to, device_id_type=MESH,
        )

    def p_copy(t):
        return pltpu.make_async_remote_copy(
            b_piece(t), bp.at[b_rows(t), :], psend.at[lax.rem(t, XD)], precv.at[t],
            device_id=p_to, device_id_type=MESH,
        )

    def q_copy(t):
        return pltpu.make_async_remote_copy(
            bx.at[b_rows(t), :], bq.at[b_rows(t), :], qsend.at[lax.rem(t, XD)], qrecv.at[t],
            device_id=p_to, device_id_type=MESH,
        )

    def place(k):
        far = 2 + jnp.where(lax.rem(k, 2) == z, 0, 1)
        return jnp.where(k // 2 == y, lax.rem(k, 2), far)

    def loads(t, slot):
        swap = 1 - 2 * lax.rem(i, 2)
        far = lax.rem(i + 2, 4)

        def a_dst(p):
            return abuf.at[slot, :, pl.ds(p * KC, KC)]

        def b_dst(k):
            return bbuf.at[slot, pl.ds(pl.multiple_of(place(k) * KC, KC), KC), :]

        def a_src(h):
            return a_ref.at[:, pl.ds(pl.multiple_of(h * m + t * KC, KC), KC)]

        pairs = [
            (a_src(0), a_dst(0)),
            (a_src(1), a_dst(1)),
            (ay.at[t], a_dst(2)),
            (b_piece(t), b_dst(i)),
            (bp.at[b_rows(t), :], b_dst(i + swap)),
            (bx.at[b_rows(t), :], b_dst(far)),
            (bq.at[b_rows(t), :], b_dst(far + swap)),
            (az.at[t], a_dst(3)),
        ]
        return [pltpu.make_async_copy(s, d, ldsem.at[slot, n]) for n, (s, d) in enumerate(pairs)]

    def compute(q, slot):
        rows = pl.ds(pl.multiple_of(q * mq, mq), mq)

        @pl.loop(0, m // tn)
        def _(n):
            cols = pl.ds(pl.multiple_of(n * tn, tn), tn)
            c_ref[rows, cols] += jnp.dot(
                abuf[slot, rows, :], bbuf[slot, :, cols], preferred_element_type=jnp.float32
            )

    barrier = pltpu.get_barrier_semaphore()
    for to in (z_to, y_to, x_to, p_to):
        pl.semaphore_signal(barrier, inc=1, device_id=to, device_id_type=MESH)
    pl.semaphore_wait(barrier, 4)

    for s in range(YD):
        y_copy(s).start()
    for t in range(XD):
        x_copy(t).start()
        p_copy(t).start()

    @pl.loop(0, m // 128)
    def _(n):
        rows = pl.ds(pl.multiple_of(n * 128, 128), 128)
        c_ref[rows, :] = jnp.zeros((128, m), jnp.float32)

    @pl.loop(0, ticks)
    def _(s):
        r, q = s // Q, lax.rem(s, Q)

        @pl.when(s >= ZD)
        def _():
            z_copy(s - ZD).wait_send()

        y_copy(s).wait_recv()
        z_copy(s).start()
        y_copy(s).wait_send()

        @pl.when(s + YD < ticks)
        def _():
            y_copy(s + YD).start()

        @pl.when((q == 1) & (r >= 1))
        def _():
            for k in range(Q):
                z_copy((r - 1) * Q + k).wait_recv()
            p_copy(r - 1).wait_recv()
            q_copy(r - 1).wait_recv()
            for ld in loads(r - 1, lax.rem(r - 1, 2)):
                ld.start()

        @pl.when(q == Q - 1)
        def _():
            @pl.when(r >= XD)
            def _():
                q_copy(r - XD).wait_send()

            x_copy(r).wait_recv()
            q_copy(r).start()
            x_copy(r).wait_send()
            p_copy(r).wait_send()

            @pl.when(r + XD < rounds)
            def _():
                x_copy(r + XD).start()
                p_copy(r + XD).start()

        @pl.when(r >= 2)
        def _():
            slot = lax.rem(r, 2)

            @pl.when(q == 0)
            def _():
                for ld in loads(r - 2, slot):
                    ld.wait()

            compute(q, slot)

    last = rounds - 1
    final = loads(last, last % 2)
    p_copy(last).wait_recv()
    for ld in final[:6]:
        ld.start()
    q_copy(last).wait_recv()
    final[6].start()
    for ld in loads(last - 1, (last - 1) % 2):
        ld.wait()

    @pl.loop(0, Q)
    def _(q):
        compute(q, (last - 1) % 2)

    for k in range(Q):
        z_copy(last * Q + k).wait_recv()
    final[7].start()
    for s in range(ticks - ZD, ticks):
        z_copy(s).wait_send()
    for t in range(rounds - XD, rounds):
        q_copy(t).wait_send()
    for ld in final:
        ld.wait()


def finish_kernel(slot, c_ref, abuf, bbuf, out, stage, sem):
    m = c_ref.shape[0]
    slots, tm, tn = stage.shape
    across = m // tn
    tiles = (m // tm) * across

    def spot(n):
        return pl.ds(pl.multiple_of(n // across * tm, tm), tm), pl.ds(pl.multiple_of(lax.rem(n, across) * tn, tn), tn)

    def write(n):
        at = lax.rem(n, slots)
        rows, cols = spot(n)
        return pltpu.make_async_copy(stage.at[at], out.at[rows, cols], sem.at[at])

    @pl.loop(0, tiles)
    def _(n):
        rows, cols = spot(n)

        @pl.when(n >= slots)
        def _():
            write(n - slots).wait()

        stage[lax.rem(n, slots)] = c_ref[rows, cols] + jnp.dot(
            abuf[slot, rows, :], bbuf[slot, :, cols], preferred_element_type=jnp.float32
        )
        write(n).start()

    for n in range(tiles - slots, tiles):
        write(n).wait()


def solution(mesh):
    def local_product(a_blk, b_blk):
        m = a_blk.shape[0]
        rounds = m // KC
        ticks = rounds * Q
        any_spec = pl.BlockSpec(memory_space=pl.ANY)
        vmem_spec = pl.BlockSpec(memory_space=pltpu.VMEM)
        dma = pltpu.SemaphoreType.DMA
        c, abuf, bbuf, *_ = pl.pallas_call(
            gather_kernel,
            name="gather",
            out_shape=(
                pltpu.VMEM((m, m), jnp.float32),
                pltpu.VMEM((2, m, 4 * KC), jnp.bfloat16),
                pltpu.VMEM((2, 4 * KC, m), jnp.bfloat16),
                pltpu.HBM((rounds, m, KC), jnp.bfloat16),
                pltpu.HBM((rounds, m, KC), jnp.bfloat16),
                pltpu.HBM((m, m), jnp.bfloat16),
                pltpu.HBM((m, m), jnp.bfloat16),
                pltpu.HBM((m, m), jnp.bfloat16),
            ),
            in_specs=[any_spec] * 2,
            out_specs=(vmem_spec,) * 3 + (any_spec,) * 5,
            scratch_shapes=[
                dma((YD,)), dma((ticks,)), dma((ZD,)), dma((ticks,)), dma((XD,)), dma((rounds,)),
                dma((XD,)), dma((rounds,)), dma((XD,)), dma((rounds,)), dma((2, 8)),
            ],
            compiler_params=pltpu.CompilerParams(
                collective_id=0, has_side_effects=True, vmem_limit_bytes=4 * 2**20
            ),
        )(a_blk, b_blk)
        c, abuf, bbuf = (pltpu.with_memory_space_constraint(v, pltpu.VMEM) for v in (c, abuf, bbuf))
        tm, tn = m // 12, m // 6
        return pl.pallas_call(
            functools.partial(finish_kernel, (rounds - 1) % 2),
            name="finish",
            out_shape=jax.ShapeDtypeStruct((m, m), jnp.float32),
            in_specs=[vmem_spec] * 3,
            out_specs=any_spec,
            scratch_shapes=[pltpu.VMEM((5, tm, tn), jnp.float32), dma((5,))],
            compiler_params=pltpu.CompilerParams(vmem_limit_bytes=4 * 2**20),
        )(c, abuf, bbuf)

    return jax.shard_map(
        local_product, mesh=mesh, in_specs=(P("row", "col"), P("row", "col")), out_specs=P("row", ("col", "dep")), check_vma=False
    )
```

```python
import functools

import jax
import jax.numpy as jnp
from jax import lax
from jax.experimental import pallas as pl
from jax.experimental.pallas import tpu as pltpu
from jax.sharding import PartitionSpec as P

MESH = pl.DeviceIdType.MESH
KC = 128
Q = 6
NT = 3
YD = 6
ZD = 6
XD = 2
LOAD = 4
AHEAD = 3
WORK = Q + 2


def gather_kernel(
    a_ref, b_ref,
    c_ref, abuf, bbuf, ay, az, bx, bp, bq,
    ysend, yrecv, zsend, zrecv, xsend, xrecv, psend, precv, qsend, qrecv, asem, bsem,
):
    z, y, i = lax.axis_index("dep"), lax.axis_index("col"), lax.axis_index("row")
    m = a_ref.shape[0]
    mq, tn = m // Q, m // NT
    rounds = m // KC
    ticks = rounds * Q
    z_to, y_to = {"dep": 1 - z}, {"col": 1 - y}
    swap = 1 - 2 * lax.rem(i, 2)
    far = lax.rem(i + 2, 4)
    x_to, p_to = {"row": far}, {"row": i + swap}

    def a_rows(s):
        return pl.ds(pl.multiple_of(lax.rem(s, Q) * mq, mq), mq)

    def a_piece(s, h):
        return a_ref.at[a_rows(s), pl.ds(pl.multiple_of(h * m + s // Q * KC, KC), KC)]

    def b_rows(t):
        return pl.ds(pl.multiple_of(t * KC, KC), KC)

    def b_piece(t):
        return b_ref.at[b_rows(t), pl.ds(pl.multiple_of(z * m, m), m)]

    def y_copy(s):
        return pltpu.make_async_remote_copy(
            a_piece(s, z), ay.at[s // Q, a_rows(s), :], ysend.at[lax.rem(s, YD)], yrecv.at[s],
            device_id=y_to, device_id_type=MESH,
        )

    def z_copy(s):
        return pltpu.make_async_remote_copy(
            ay.at[s // Q, a_rows(s), :], az.at[s // Q, a_rows(s), :], zsend.at[lax.rem(s, ZD)], zrecv.at[s],
            device_id=z_to, device_id_type=MESH,
        )

    def x_copy(t):
        return pltpu.make_async_remote_copy(
            b_piece(t), bx.at[b_rows(t), :], xsend.at[lax.rem(t, XD)], xrecv.at[t],
            device_id=x_to, device_id_type=MESH,
        )

    def p_copy(t):
        return pltpu.make_async_remote_copy(
            b_piece(t), bp.at[b_rows(t), :], psend.at[lax.rem(t, XD)], precv.at[t],
            device_id=p_to, device_id_type=MESH,
        )

    def q_copy(t):
        return pltpu.make_async_remote_copy(
            bx.at[b_rows(t), :], bq.at[b_rows(t), :], qsend.at[lax.rem(t, XD)], qrecv.at[t],
            device_id=p_to, device_id_type=MESH,
        )

    def place(k):
        return jnp.where(k // 2 == y, lax.rem(k, 2), 2 + jnp.where(lax.rem(k, 2) == z, 0, 1))

    def a_loads(s):
        slot = lax.rem(s // Q, 2)
        sources = [a_piece(s, 0), a_piece(s, 1), ay.at[s // Q, a_rows(s), :], az.at[s // Q, a_rows(s), :]]
        return [
            pltpu.make_async_copy(
                src, abuf.at[slot, a_rows(s), pl.ds(p * KC, KC)], asem.at[lax.rem(s, AHEAD + Q), p]
            )
            for p, src in enumerate(sources)
        ]

    def b_loads(t):
        slot = lax.rem(t, 2)
        sources = [
            (b_piece(t), i),
            (bp.at[b_rows(t), :], i + swap),
            (bx.at[b_rows(t), :], far),
            (bq.at[b_rows(t), :], far + swap),
        ]
        return [
            pltpu.make_async_copy(
                src, bbuf.at[slot, pl.ds(pl.multiple_of(place(k) * KC, KC), KC), :], bsem.at[slot, n]
            )
            for n, (src, k) in enumerate(sources)
        ]

    def compute(s):
        slot, rows = lax.rem(s // Q, 2), a_rows(s)
        for n in range(NT):
            cols = pl.ds(n * tn, tn)
            c_ref[rows, cols] += jnp.dot(
                abuf[slot, rows, :], bbuf[slot, :, cols], preferred_element_type=jnp.float32
            )

    barrier = pltpu.get_barrier_semaphore()
    for to in (z_to, y_to, x_to, p_to):
        pl.semaphore_signal(barrier, inc=1, device_id=to, device_id_type=MESH)
    pl.semaphore_wait(barrier, 4)

    for s in range(YD):
        y_copy(s).start()
    for t in range(XD):
        x_copy(t).start()
        p_copy(t).start()

    @pl.loop(0, m // 128)
    def _(n):
        rows = pl.ds(pl.multiple_of(n * 128, 128), 128)
        c_ref[rows, :] = jnp.zeros((128, m), jnp.float32)

    def work(s):
        for ld in a_loads(s):
            ld.wait()

        @pl.when(lax.rem(s, Q) == 0)
        def _():
            for ld in b_loads(s // Q):
                ld.wait()

        compute(s)

    def load(s):
        z_copy(s).wait_recv()
        for ld in a_loads(s):
            ld.start()

    @pl.loop(0, ticks + WORK - Q)
    def _(s):
        r, q = s // Q, lax.rem(s, Q)

        @pl.when(s < ticks)
        def _():
            @pl.when(s >= ZD)
            def _():
                z_copy(s - ZD).wait_send()

            y_copy(s).wait_recv()
            z_copy(s).start()
            y_copy(s).wait_send()

            @pl.when(s + YD < ticks)
            def _():
                y_copy(s + YD).start()

            @pl.when(q == Q - 1)
            def _():
                @pl.when(r >= XD)
                def _():
                    q_copy(r - XD).wait_send()

                x_copy(r).wait_recv()
                q_copy(r).start()
                x_copy(r).wait_send()
                p_copy(r).wait_send()

                @pl.when(r + XD < rounds)
                def _():
                    x_copy(r + XD).start()
                    p_copy(r + XD).start()

        @pl.when((q == 1) & (r >= 1))
        def _():
            p_copy(r - 1).wait_recv()
            q_copy(r - 1).wait_recv()
            for ld in b_loads(r - 1):
                ld.start()

        @pl.when((s >= LOAD) & (s - LOAD < ticks))
        def _():
            load(s - LOAD)

        @pl.when(s >= WORK)
        def _():
            work(s - WORK)

    for s in range(ticks + WORK - Q - LOAD, ticks):
        load(s)
    for s in range(ticks - ZD, ticks):
        z_copy(s).wait_send()
    for t in range(rounds - XD, rounds):
        q_copy(t).wait_send()
    for s in range(ticks - Q, ticks):
        for ld in a_loads(s):
            ld.wait()
    for ld in b_loads(rounds - 1):
        ld.wait()


def finish_kernel(slot, c_ref, abuf, bbuf, out, total, sem):
    m = c_ref.shape[0]
    tm, tn = m // Q, m // NT

    def write(k, n):
        at = pl.ds(pl.multiple_of(k * tm, tm), tm), pl.ds(n * tn, tn)
        return pltpu.make_async_copy(total.at[at], out.at[at], sem.at[k, n])

    @pl.loop(0, Q)
    def _(k):
        rows = pl.ds(pl.multiple_of(k * tm, tm), tm)
        for n in range(NT):
            cols = pl.ds(n * tn, tn)
            total[rows, cols] = c_ref[rows, cols] + jnp.dot(
                abuf[slot, rows, :], bbuf[slot, :, cols], preferred_element_type=jnp.float32
            )
            write(k, n).start()

    @pl.loop(0, Q)
    def _(k):
        for n in range(NT):
            write(k, n).wait()


def solution(mesh):
    def local_product(a_blk, b_blk):
        m = a_blk.shape[0]
        rounds = m // KC
        ticks = rounds * Q
        any_spec = pl.BlockSpec(memory_space=pl.ANY)
        vmem_spec = pl.BlockSpec(memory_space=pltpu.VMEM)
        dma = pltpu.SemaphoreType.DMA
        c, abuf, bbuf, *_ = pl.pallas_call(
            gather_kernel,
            name="gather",
            out_shape=(
                pltpu.VMEM((m, m), jnp.float32),
                pltpu.VMEM((2, m, 4 * KC), jnp.bfloat16),
                pltpu.VMEM((2, 4 * KC, m), jnp.bfloat16),
                pltpu.HBM((rounds, m, KC), jnp.bfloat16),
                pltpu.HBM((rounds, m, KC), jnp.bfloat16),
                pltpu.HBM((m, m), jnp.bfloat16),
                pltpu.HBM((m, m), jnp.bfloat16),
                pltpu.HBM((m, m), jnp.bfloat16),
            ),
            in_specs=[any_spec] * 2,
            out_specs=(vmem_spec,) * 3 + (any_spec,) * 5,
            scratch_shapes=[
                dma((YD,)), dma((ticks,)), dma((ZD,)), dma((ticks,)), dma((XD,)), dma((rounds,)),
                dma((XD,)), dma((rounds,)), dma((XD,)), dma((rounds,)), dma((AHEAD + Q, 4)), dma((2, 4)),
            ],
            compiler_params=pltpu.CompilerParams(
                collective_id=0, has_side_effects=True, vmem_limit_bytes=4 * 2**20
            ),
        )(a_blk, b_blk)
        c, abuf, bbuf = (pltpu.with_memory_space_constraint(v, pltpu.VMEM) for v in (c, abuf, bbuf))
        return pl.pallas_call(
            functools.partial(finish_kernel, (rounds - 1) % 2),
            name="finish",
            out_shape=(jax.ShapeDtypeStruct((m, m), jnp.float32), pltpu.VMEM((m, m), jnp.float32)),
            in_specs=[vmem_spec] * 3,
            out_specs=(any_spec, vmem_spec),
            input_output_aliases={0: 1},
            scratch_shapes=[dma((Q, NT))],
            compiler_params=pltpu.CompilerParams(vmem_limit_bytes=4 * 2**20),
        )(c, abuf, bbuf)[0]

    return jax.shard_map(
        local_product, mesh=mesh, in_specs=(P("row", "col"), P("row", "col")), out_specs=P("row", ("col", "dep")), check_vma=False
    )
```

```python
import functools

import jax
import jax.numpy as jnp
from jax import lax
from jax.experimental import pallas as pl
from jax.experimental.pallas import tpu as pltpu
from jax.sharding import PartitionSpec as P

MESH = pl.DeviceIdType.MESH
KC = 128
Q = 6
NT = 3
YD = 6
ZD = 6
HALF = KC // 2
XD = 4
PD = 2
LOAD = 4
AHEAD = 3
WORK = Q + 1


def gather_kernel(
    a_ref, b_ref,
    c_ref, abuf, bbuf, ay, az, bx, bp, bq,
    ysend, yrecv, zsend, zrecv, wsend, xsend, xrecv, psend, precv, qsend, qrecv, asem, bsem, yfree, zfree, pfree,
):
    z, y, i = lax.axis_index("dep"), lax.axis_index("col"), lax.axis_index("row")
    m = a_ref.shape[0]
    mq, tn = m // Q, m // NT
    rounds = m // KC
    ticks, halves = rounds * Q, 2 * rounds
    last_slot = (rounds - 1) % 2
    z_to, y_to = {"dep": 1 - z}, {"col": 1 - y}
    swap = 1 - 2 * lax.rem(i, 2)
    far = lax.rem(i + 2, 4)
    x_to, p_to = {"row": far}, {"row": i + swap}

    def a_rows(s):
        return pl.ds(pl.multiple_of(lax.rem(s, Q) * mq, mq), mq)

    def a_piece(s, h):
        return a_ref.at[a_rows(s), pl.ds(pl.multiple_of(h * m + s // Q * KC, KC), KC)]

    def b_rows(t):
        return pl.ds(pl.multiple_of(t * KC, KC), KC)

    def b_piece(t):
        return b_ref.at[b_rows(t), pl.ds(pl.multiple_of(z * m, m), m)]

    def y_copy(s):
        return pltpu.make_async_remote_copy(
            a_piece(s, z), ay.at[s // Q, a_rows(s), :], ysend.at[lax.rem(s, YD)], yrecv.at[s],
            device_id=y_to, device_id_type=MESH,
        )

    def z_copy(s):
        return pltpu.make_async_remote_copy(
            ay.at[s // Q, a_rows(s), :], az.at[s // Q, a_rows(s), :], zsend.at[lax.rem(s, ZD)], zrecv.at[s],
            device_id=z_to, device_id_type=MESH,
        )

    def z_direct(s):
        return pltpu.make_async_remote_copy(
            ay.at[s // Q, a_rows(s), :], abuf.at[last_slot, a_rows(s), pl.ds(3 * KC, KC)],
            zsend.at[lax.rem(s, ZD)], zrecv.at[s],
            device_id=z_to, device_id_type=MESH,
        )

    def w_copy():
        s = ticks - 1
        return pltpu.make_async_remote_copy(
            a_piece(s, 1 - z), abuf.at[last_slot, a_rows(s), pl.ds(3 * KC, KC)], wsend, zrecv.at[s],
            device_id=y_to, device_id_type=MESH,
        )

    def half_rows(u):
        return pl.ds(pl.multiple_of(u * HALF, HALF), HALF)

    def x_copy(u):
        return pltpu.make_async_remote_copy(
            b_ref.at[half_rows(u), pl.ds(pl.multiple_of(z * m, m), m)], bx.at[half_rows(u), :],
            xsend.at[lax.rem(u, XD)], xrecv.at[u],
            device_id=x_to, device_id_type=MESH,
        )

    def p_copy(t):
        return pltpu.make_async_remote_copy(
            b_piece(t), bp.at[b_rows(t), :], psend.at[lax.rem(t, PD)], precv.at[t],
            device_id=p_to, device_id_type=MESH,
        )

    def q_copy(u):
        return pltpu.make_async_remote_copy(
            bx.at[half_rows(u), :], bq.at[half_rows(u), :], qsend.at[lax.rem(u, XD)], qrecv.at[u],
            device_id=p_to, device_id_type=MESH,
        )

    def q_direct(u):
        rows = pl.ds(pl.multiple_of(place(far) * KC + lax.rem(u, 2) * HALF, HALF), HALF)
        return pltpu.make_async_remote_copy(
            bx.at[half_rows(u), :], bbuf.at[last_slot, rows, :], qsend.at[lax.rem(u, XD)], qrecv.at[u],
            device_id=p_to, device_id_type=MESH,
        )

    def place(k):
        return jnp.where(k // 2 == y, lax.rem(k, 2), 2 + jnp.where(lax.rem(k, 2) == z, 0, 1))

    def a_loads(s, parts=range(4)):
        slot = lax.rem(s // Q, 2)
        sources = [a_piece(s, 0), a_piece(s, 1), ay.at[s // Q, a_rows(s), :], az.at[s // Q, a_rows(s), :]]
        return [
            pltpu.make_async_copy(
                sources[p], abuf.at[slot, a_rows(s), pl.ds(p * KC, KC)], asem.at[lax.rem(s, AHEAD + Q), p]
            )
            for p in parts
        ]

    def b_loads(t, parts=range(4)):
        slot = lax.rem(t, 2)
        sources = [
            (b_piece(t), i),
            (bp.at[b_rows(t), :], i + swap),
            (bx.at[b_rows(t), :], far),
            (bq.at[b_rows(t), :], far + swap),
        ]
        return [
            pltpu.make_async_copy(
                sources[n][0],
                bbuf.at[slot, pl.ds(pl.multiple_of(place(sources[n][1]) * KC, KC), KC), :],
                bsem.at[slot, n],
            )
            for n in parts
        ]

    def compute(s):
        slot, rows = lax.rem(s // Q, 2), a_rows(s)
        for n in range(NT):
            cols = pl.ds(n * tn, tn)
            c_ref[rows, cols] += jnp.dot(
                abuf[slot, rows, :], bbuf[slot, :, cols], preferred_element_type=jnp.float32
            )

    barrier = pltpu.get_barrier_semaphore()
    for to in (z_to, y_to, x_to, p_to):
        pl.semaphore_signal(barrier, inc=1, device_id=to, device_id_type=MESH)
    pl.semaphore_wait(barrier, 4)

    for s in range(YD):
        y_copy(s).start()
    for u in range(XD):
        x_copy(u).start()
    for t in range(PD):
        p_copy(t).start()

    @pl.loop(0, m // 128)
    def _(n):
        rows = pl.ds(pl.multiple_of(n * 128, 128), 128)
        c_ref[rows, :] = jnp.zeros((128, m), jnp.float32)

    def work(s):
        for ld in a_loads(s):
            ld.wait()

        @pl.when(lax.rem(s, Q) == 0)
        def _():
            for ld in b_loads(s // Q):
                ld.wait()

        compute(s)

    def load(s):
        z_copy(s).wait_recv()
        for ld in a_loads(s):
            ld.start()

    @pl.loop(0, ticks)
    def _(s):
        r, q = s // Q, lax.rem(s, Q)

        @pl.when(s >= ZD)
        def _():
            z_copy(s - ZD).wait_send()

        y_copy(s).wait_recv()

        @pl.when(s < ticks - 2)
        def _():
            z_copy(s).start()

        @pl.when(s == ticks - 2)
        def _():
            pl.semaphore_wait(zfree, 1)
            z_direct(s).start()

        y_copy(s).wait_send()

        @pl.when(s + YD < ticks)
        def _():
            y_copy(s + YD).start()

        @pl.when(s == ticks - 3)
        def _():
            pl.semaphore_wait(yfree, 1)
            w_copy().start()

        @pl.when(lax.rem(q, Q // 2) == Q // 2 - 1)
        def _():
            u = s // (Q // 2)

            @pl.when(u >= XD)
            def _():
                q_copy(u - XD).wait_send()

            x_copy(u).wait_recv()

            @pl.when(u < halves - 2)
            def _():
                q_copy(u).start()

            @pl.when(u == halves - 2)
            def _():
                pl.semaphore_wait(pfree, 1)

            @pl.when(u >= halves - 2)
            def _():
                q_direct(u).start()

            x_copy(u).wait_send()

            @pl.when(u + XD < halves)
            def _():
                x_copy(u + XD).start()

        @pl.when(q == Q - 1)
        def _():
            p_copy(r).wait_send()

            @pl.when(r + PD < rounds)
            def _():
                p_copy(r + PD).start()

        @pl.when(s >= LOAD)
        def _():
            load(s - LOAD)

        @pl.when(s >= WORK)
        def _():
            work(s - WORK)

        @pl.when((q == 0) & (r >= 1))
        def _():
            p_copy(r - 1).wait_recv()
            q_copy(2 * r - 2).wait_recv()
            q_copy(2 * r - 1).wait_recv()
            for ld in b_loads(r - 1):
                ld.start()

        @pl.when(s == ticks - Q)
        def _():
            for free, to in ((yfree, y_to), (zfree, z_to), (pfree, p_to)):
                pl.semaphore_signal(free, inc=1, device_id=to, device_id_type=MESH)

    load(ticks - 4)
    for s in range(ticks - 3, ticks):
        for ld in a_loads(s, range(3)):
            ld.start()
    p_copy(rounds - 1).wait_recv()
    for ld in b_loads(rounds - 1, range(3)):
        ld.start()
    work(ticks - WORK)
    z_copy(ticks - 3).wait_recv()
    a_loads(ticks - 3, [3])[0].start()
    for s in range(ticks - ZD, ticks - 1):
        z_copy(s).wait_send()
    w_copy().wait_send()
    for u in range(halves - XD, halves):
        q_copy(u).wait_send()
    for s in range(ticks - Q, ticks - 2):
        for ld in a_loads(s):
            ld.wait()
    for s in range(ticks - 2, ticks):
        for ld in a_loads(s, range(3)):
            ld.wait()
    for ld in b_loads(rounds - 1, range(3)):
        ld.wait()
    for u in range(halves - 2, halves):
        q_copy(u).wait_recv()
    for s in range(ticks - 2, ticks):
        z_copy(s).wait_recv()


def finish_kernel(slot, c_ref, abuf, bbuf, out, total, sem):
    m = c_ref.shape[0]
    tm, tn = m // Q, m // NT

    def write(k, n):
        at = pl.ds(pl.multiple_of(k * tm, tm), tm), pl.ds(n * tn, tn)
        return pltpu.make_async_copy(total.at[at], out.at[at], sem.at[k, n])

    @pl.loop(0, Q)
    def _(k):
        rows = pl.ds(pl.multiple_of(k * tm, tm), tm)
        for n in range(NT):
            cols = pl.ds(n * tn, tn)
            total[rows, cols] = c_ref[rows, cols] + jnp.dot(
                abuf[slot, rows, :], bbuf[slot, :, cols], preferred_element_type=jnp.float32
            )
            write(k, n).start()

    @pl.loop(0, Q)
    def _(k):
        for n in range(NT):
            write(k, n).wait()


def solution(mesh):
    def local_product(a_blk, b_blk):
        m = a_blk.shape[0]
        rounds = m // KC
        ticks = rounds * Q
        any_spec = pl.BlockSpec(memory_space=pl.ANY)
        vmem_spec = pl.BlockSpec(memory_space=pltpu.VMEM)
        dma = pltpu.SemaphoreType.DMA
        c, abuf, bbuf, *_ = pl.pallas_call(
            gather_kernel,
            name="gather",
            out_shape=(
                pltpu.VMEM((m, m), jnp.float32),
                pltpu.VMEM((2, m, 4 * KC), jnp.bfloat16),
                pltpu.VMEM((2, 4 * KC, m), jnp.bfloat16),
                pltpu.HBM((rounds, m, KC), jnp.bfloat16),
                pltpu.HBM((rounds, m, KC), jnp.bfloat16),
                pltpu.HBM((m, m), jnp.bfloat16),
                pltpu.HBM((m, m), jnp.bfloat16),
                pltpu.HBM((m, m), jnp.bfloat16),
            ),
            in_specs=[any_spec] * 2,
            out_specs=(vmem_spec,) * 3 + (any_spec,) * 5,
            scratch_shapes=[
                dma((YD,)), dma((ticks,)), dma((ZD,)), dma((ticks,)), dma, dma((XD,)), dma((2 * rounds,)),
                dma((PD,)), dma((rounds,)), dma((XD,)), dma((2 * rounds,)), dma((AHEAD + Q, 4)), dma((2, 4)),
                *[pltpu.SemaphoreType.REGULAR] * 3,
            ],
            compiler_params=pltpu.CompilerParams(
                collective_id=0, has_side_effects=True, vmem_limit_bytes=4 * 2**20
            ),
        )(a_blk, b_blk)
        c, abuf, bbuf = (pltpu.with_memory_space_constraint(v, pltpu.VMEM) for v in (c, abuf, bbuf))
        return pl.pallas_call(
            functools.partial(finish_kernel, (rounds - 1) % 2),
            name="finish",
            out_shape=(jax.ShapeDtypeStruct((m, m), jnp.float32), pltpu.VMEM((m, m), jnp.float32)),
            in_specs=[vmem_spec] * 3,
            out_specs=(any_spec, vmem_spec),
            input_output_aliases={0: 1},
            scratch_shapes=[dma((Q, NT))],
            compiler_params=pltpu.CompilerParams(vmem_limit_bytes=4 * 2**20),
        )(c, abuf, bbuf)[0]

    return jax.shard_map(
        local_product, mesh=mesh, in_specs=(P("row", "col"), P("row", "col")), out_specs=P("row", ("col", "dep")), check_vma=False
    )
```

```python
import functools

import jax
import jax.numpy as jnp
from jax import lax
from jax.experimental import pallas as pl
from jax.experimental.pallas import tpu as pltpu
from jax.sharding import PartitionSpec as P

MESH = pl.DeviceIdType.MESH
KC = 128
Q = 6
NT = 3
YD = 6
ZD = 6
HALF = KC // 2
XD = 4
PD = 2
LOAD = 4
AHEAD = 3
WORK = Q + 1


def gather_kernel(
    a_ref, b_ref,
    c_ref, abuf, bbuf, ay, az, bx, bp, bq,
    ysend, yrecv, zsend, zrecv, wsend, xsend, xrecv, psend, precv, qsend, qrecv, asem, bsem, yfree, zfree, pfree,
):
    z, y, i = lax.axis_index("dep"), lax.axis_index("col"), lax.axis_index("row")
    m = a_ref.shape[0]
    mq, tn = m // Q, m // NT
    rounds = m // KC
    ticks, halves = rounds * Q, 2 * rounds
    last_slot = (rounds - 1) % 2
    z_to, y_to = {"dep": 1 - z}, {"col": 1 - y}
    swap = 1 - 2 * lax.rem(i, 2)
    far = lax.rem(i + 2, 4)
    x_to, p_to = {"row": far}, {"row": i + swap}

    def a_rows(s):
        return pl.ds(pl.multiple_of(lax.rem(s, Q) * mq, mq), mq)

    def a_piece(s, h):
        return a_ref.at[a_rows(s), pl.ds(pl.multiple_of(h * m + s // Q * KC, KC), KC)]

    def b_rows(t):
        return pl.ds(pl.multiple_of(t * KC, KC), KC)

    def b_piece(t):
        return b_ref.at[b_rows(t), pl.ds(pl.multiple_of(z * m, m), m)]

    def y_copy(s):
        return pltpu.make_async_remote_copy(
            a_piece(s, z), ay.at[s // Q, a_rows(s), :], ysend.at[lax.rem(s, YD)], yrecv.at[s],
            device_id=y_to, device_id_type=MESH,
        )

    def z_copy(s):
        return pltpu.make_async_remote_copy(
            ay.at[s // Q, a_rows(s), :], az.at[s // Q, a_rows(s), :], zsend.at[lax.rem(s, ZD)], zrecv.at[s],
            device_id=z_to, device_id_type=MESH,
        )

    def z_direct(s):
        return pltpu.make_async_remote_copy(
            ay.at[s // Q, a_rows(s), :], abuf.at[last_slot, a_rows(s), pl.ds(3 * KC, KC)],
            zsend.at[lax.rem(s, ZD)], zrecv.at[s],
            device_id=z_to, device_id_type=MESH,
        )

    def w_copy():
        s = ticks - 1
        return pltpu.make_async_remote_copy(
            a_piece(s, 1 - z), abuf.at[last_slot, a_rows(s), pl.ds(3 * KC, KC)], wsend, zrecv.at[s],
            device_id=y_to, device_id_type=MESH,
        )

    def half_rows(u):
        return pl.ds(pl.multiple_of(u * HALF, HALF), HALF)

    def x_copy(u):
        return pltpu.make_async_remote_copy(
            b_ref.at[half_rows(u), pl.ds(pl.multiple_of(z * m, m), m)], bx.at[half_rows(u), :],
            xsend.at[lax.rem(u, XD)], xrecv.at[u],
            device_id=x_to, device_id_type=MESH,
        )

    def p_copy(t):
        return pltpu.make_async_remote_copy(
            b_piece(t), bp.at[b_rows(t), :], psend.at[lax.rem(t, PD)], precv.at[t],
            device_id=p_to, device_id_type=MESH,
        )

    def q_copy(u):
        return pltpu.make_async_remote_copy(
            bx.at[half_rows(u), :], bq.at[half_rows(u), :], qsend.at[lax.rem(u, XD)], qrecv.at[u],
            device_id=p_to, device_id_type=MESH,
        )

    def q_direct(u):
        rows = pl.ds(pl.multiple_of(place(far) * KC + lax.rem(u, 2) * HALF, HALF), HALF)
        return pltpu.make_async_remote_copy(
            bx.at[half_rows(u), :], bbuf.at[last_slot, rows, :], qsend.at[lax.rem(u, XD)], qrecv.at[u],
            device_id=p_to, device_id_type=MESH,
        )

    def place(k):
        return jnp.where(k // 2 == y, lax.rem(k, 2), 2 + jnp.where(lax.rem(k, 2) == z, 0, 1))

    def a_loads(s, parts=range(4)):
        slot = lax.rem(s // Q, 2)
        sources = [a_piece(s, 0), a_piece(s, 1), ay.at[s // Q, a_rows(s), :], az.at[s // Q, a_rows(s), :]]
        return [
            pltpu.make_async_copy(
                sources[p], abuf.at[slot, a_rows(s), pl.ds(p * KC, KC)], asem.at[lax.rem(s, AHEAD + Q), p]
            )
            for p in parts
        ]

    def b_loads(t, parts=range(4)):
        slot = lax.rem(t, 2)
        sources = [
            (b_piece(t), i),
            (bp.at[b_rows(t), :], i + swap),
            (bx.at[b_rows(t), :], far),
            (bq.at[b_rows(t), :], far + swap),
        ]
        return [
            pltpu.make_async_copy(
                sources[n][0],
                bbuf.at[slot, pl.ds(pl.multiple_of(place(sources[n][1]) * KC, KC), KC), :],
                bsem.at[slot, n],
            )
            for n in parts
        ]

    def compute(s):
        slot, rows = lax.rem(s // Q, 2), a_rows(s)
        for n in range(NT):
            cols = pl.ds(n * tn, tn)
            c_ref[rows, cols] += jnp.dot(
                abuf[slot, rows, :], bbuf[slot, :, cols], preferred_element_type=jnp.float32
            )

    barrier = pltpu.get_barrier_semaphore()
    for to in (z_to, y_to, x_to, p_to):
        pl.semaphore_signal(barrier, inc=1, device_id=to, device_id_type=MESH)
    pl.semaphore_wait(barrier, 4)

    for s in range(YD):
        y_copy(s).start()
    for u in range(XD):
        x_copy(u).start()
    for t in range(PD):
        p_copy(t).start()

    @pl.loop(0, m // 128)
    def _(n):
        rows = pl.ds(pl.multiple_of(n * 128, 128), 128)
        c_ref[rows, :] = jnp.zeros((128, m), jnp.float32)

    def work(s):
        for ld in a_loads(s):
            ld.wait()

        @pl.when(lax.rem(s, Q) == 0)
        def _():
            for ld in b_loads(s // Q):
                ld.wait()

        compute(s)

    def load(s):
        z_copy(s).wait_recv()
        for ld in a_loads(s):
            ld.start()

    @pl.loop(0, ticks)
    def _(s):
        r, q = s // Q, lax.rem(s, Q)

        @pl.when(s >= ZD)
        def _():
            z_copy(s - ZD).wait_send()

        y_copy(s).wait_recv()

        @pl.when(s < ticks - 2)
        def _():
            z_copy(s).start()

        @pl.when(s == ticks - 2)
        def _():
            pl.semaphore_wait(zfree, 1)
            z_direct(s).start()

        y_copy(s).wait_send()

        @pl.when(s + YD < ticks)
        def _():
            y_copy(s + YD).start()

        @pl.when(s == ticks - 3)
        def _():
            pl.semaphore_wait(yfree, 1)
            w_copy().start()

        @pl.when(lax.rem(q, Q // 2) == Q // 2 - 1)
        def _():
            u = s // (Q // 2)

            @pl.when(u >= XD)
            def _():
                q_copy(u - XD).wait_send()

            x_copy(u).wait_recv()

            @pl.when(u < halves - 2)
            def _():
                q_copy(u).start()

            @pl.when(u == halves - 2)
            def _():
                pl.semaphore_wait(pfree, 1)

            @pl.when(u >= halves - 2)
            def _():
                q_direct(u).start()

            x_copy(u).wait_send()

            @pl.when(u + XD < halves)
            def _():
                x_copy(u + XD).start()

        @pl.when(q == Q - 1)
        def _():
            p_copy(r).wait_send()

            @pl.when(r + PD < rounds)
            def _():
                p_copy(r + PD).start()

        @pl.when(s >= LOAD)
        def _():
            load(s - LOAD)

        @pl.when((q == 0) & (r >= 1))
        def _():
            p_copy(r - 1).wait_recv()
            q_copy(2 * r - 2).wait_recv()
            q_copy(2 * r - 1).wait_recv()
            for ld in b_loads(r - 1):
                ld.start()

        @pl.when(s >= WORK)
        def _():
            work(s - WORK)

        @pl.when(s == ticks - Q)
        def _():
            for free, to in ((yfree, y_to), (zfree, z_to), (pfree, p_to)):
                pl.semaphore_signal(free, inc=1, device_id=to, device_id_type=MESH)

    load(ticks - 4)
    for s in range(ticks - 3, ticks):
        for ld in a_loads(s, range(3)):
            ld.start()
    p_copy(rounds - 1).wait_recv()
    for ld in b_loads(rounds - 1, range(3)):
        ld.start()
    work(ticks - WORK)
    z_copy(ticks - 3).wait_recv()
    a_loads(ticks - 3, [3])[0].start()
    for s in range(ticks - ZD, ticks - 1):
        z_copy(s).wait_send()
    w_copy().wait_send()
    for u in range(halves - XD, halves):
        q_copy(u).wait_send()
    for s in range(ticks - Q, ticks - 2):
        for ld in a_loads(s):
            ld.wait()
    for s in range(ticks - 2, ticks):
        for ld in a_loads(s, range(3)):
            ld.wait()
    for ld in b_loads(rounds - 1, range(3)):
        ld.wait()
    for u in range(halves - 2, halves):
        q_copy(u).wait_recv()
    for s in range(ticks - 2, ticks):
        z_copy(s).wait_recv()


def finish_kernel(slot, c_ref, abuf, bbuf, out, total, sem):
    m = c_ref.shape[0]
    tm, tn = m // Q, m // NT

    def write(k, n):
        at = pl.ds(k * tm, tm), pl.ds(n * tn, tn)
        return pltpu.make_async_copy(total.at[at], out.at[at], sem.at[k, n])

    for k in range(Q):
        rows = pl.ds(k * tm, tm)
        for n in range(NT):
            cols = pl.ds(n * tn, tn)
            total[rows, cols] = c_ref[rows, cols] + jnp.dot(
                abuf[slot, rows, :], bbuf[slot, :, cols], preferred_element_type=jnp.float32
            )
            write(k, n).start()
    for k in range(Q):
        for n in range(NT):
            write(k, n).wait()


def solution(mesh):
    def local_product(a_blk, b_blk):
        m = a_blk.shape[0]
        rounds = m // KC
        ticks = rounds * Q
        any_spec = pl.BlockSpec(memory_space=pl.ANY)
        vmem_spec = pl.BlockSpec(memory_space=pltpu.VMEM)
        dma = pltpu.SemaphoreType.DMA
        c, abuf, bbuf, *_ = pl.pallas_call(
            gather_kernel,
            name="gather",
            out_shape=(
                pltpu.VMEM((m, m), jnp.float32),
                pltpu.VMEM((2, m, 4 * KC), jnp.bfloat16),
                pltpu.VMEM((2, 4 * KC, m), jnp.bfloat16),
                pltpu.HBM((rounds, m, KC), jnp.bfloat16),
                pltpu.HBM((rounds, m, KC), jnp.bfloat16),
                pltpu.HBM((m, m), jnp.bfloat16),
                pltpu.HBM((m, m), jnp.bfloat16),
                pltpu.HBM((m, m), jnp.bfloat16),
            ),
            in_specs=[any_spec] * 2,
            out_specs=(vmem_spec,) * 3 + (any_spec,) * 5,
            scratch_shapes=[
                dma((YD,)), dma((ticks,)), dma((ZD,)), dma((ticks,)), dma, dma((XD,)), dma((2 * rounds,)),
                dma((PD,)), dma((rounds,)), dma((XD,)), dma((2 * rounds,)), dma((AHEAD + Q, 4)), dma((2, 4)),
                *[pltpu.SemaphoreType.REGULAR] * 3,
            ],
            compiler_params=pltpu.CompilerParams(
                collective_id=0, has_side_effects=True, vmem_limit_bytes=4 * 2**20
            ),
        )(a_blk, b_blk)
        c, abuf, bbuf = (pltpu.with_memory_space_constraint(v, pltpu.VMEM) for v in (c, abuf, bbuf))
        return pl.pallas_call(
            functools.partial(finish_kernel, (rounds - 1) % 2),
            name="finish",
            out_shape=(jax.ShapeDtypeStruct((m, m), jnp.float32), pltpu.VMEM((m, m), jnp.float32)),
            in_specs=[vmem_spec] * 3,
            out_specs=(any_spec, vmem_spec),
            input_output_aliases={0: 1},
            scratch_shapes=[dma((Q, NT))],
            compiler_params=pltpu.CompilerParams(vmem_limit_bytes=4 * 2**20),
        )(c, abuf, bbuf)[0]

    return jax.shard_map(
        local_product, mesh=mesh, in_specs=(P("row", "col"), P("row", "col")), out_specs=P("row", ("col", "dep")), check_vma=False
    )
```

```python
import functools

import jax
import jax.numpy as jnp
from jax import lax
from jax.experimental import pallas as pl
from jax.experimental.pallas import tpu as pltpu
from jax.sharding import PartitionSpec as P

MESH = pl.DeviceIdType.MESH
KC = 128
Q = 6
NT = 3
YD = 6
ZD = 6
HALF = KC // 2
XD = 4
PD = 2
LOAD = 4
AHEAD = 3
WORK = Q + 1


def rem(a, b):
    return a % b if isinstance(a, int) else lax.rem(a, b)


def gather_kernel(
    a_ref, b_ref,
    c_ref, abuf, bbuf, ay, az, bx, bp, bq,
    ysend, yrecv, zsend, zrecv, wsend, xsend, xrecv, psend, precv, qsend, qrecv, asem, bsem, yfree, zfree, pfree,
):
    z, y, i = lax.axis_index("dep"), lax.axis_index("col"), lax.axis_index("row")
    m = a_ref.shape[0]
    mq, tn = m // Q, m // NT
    rounds = m // KC
    ticks, halves = rounds * Q, 2 * rounds
    last_slot = (rounds - 1) % 2
    z_to, y_to = {"dep": 1 - z}, {"col": 1 - y}
    swap = 1 - 2 * rem(i, 2)
    far = rem(i + 2, 4)
    x_to, p_to = {"row": far}, {"row": i + swap}

    def a_rows(s):
        return pl.ds(pl.multiple_of(rem(s, Q) * mq, mq), mq)

    def a_piece(s, h):
        return a_ref.at[a_rows(s), pl.ds(pl.multiple_of(h * m + s // Q * KC, KC), KC)]

    def b_rows(t):
        return pl.ds(pl.multiple_of(t * KC, KC), KC)

    def b_piece(t):
        return b_ref.at[b_rows(t), pl.ds(pl.multiple_of(z * m, m), m)]

    def y_copy(s):
        return pltpu.make_async_remote_copy(
            a_piece(s, z), ay.at[s // Q, a_rows(s), :], ysend.at[rem(s, YD)], yrecv.at[s],
            device_id=y_to, device_id_type=MESH,
        )

    def z_copy(s):
        return pltpu.make_async_remote_copy(
            ay.at[s // Q, a_rows(s), :], az.at[s // Q, a_rows(s), :], zsend.at[rem(s, ZD)], zrecv.at[s],
            device_id=z_to, device_id_type=MESH,
        )

    def z_direct(s):
        return pltpu.make_async_remote_copy(
            ay.at[s // Q, a_rows(s), :], abuf.at[last_slot, a_rows(s), pl.ds(3 * KC, KC)],
            zsend.at[rem(s, ZD)], zrecv.at[s],
            device_id=z_to, device_id_type=MESH,
        )

    def w_copy():
        s = ticks - 1
        return pltpu.make_async_remote_copy(
            a_piece(s, 1 - z), abuf.at[last_slot, a_rows(s), pl.ds(3 * KC, KC)], wsend, zrecv.at[s],
            device_id=y_to, device_id_type=MESH,
        )

    def half_rows(u):
        return pl.ds(pl.multiple_of(u * HALF, HALF), HALF)

    def x_copy(u):
        return pltpu.make_async_remote_copy(
            b_ref.at[half_rows(u), pl.ds(pl.multiple_of(z * m, m), m)], bx.at[half_rows(u), :],
            xsend.at[rem(u, XD)], xrecv.at[u],
            device_id=x_to, device_id_type=MESH,
        )

    def p_copy(t):
        return pltpu.make_async_remote_copy(
            b_piece(t), bp.at[b_rows(t), :], psend.at[rem(t, PD)], precv.at[t],
            device_id=p_to, device_id_type=MESH,
        )

    def q_copy(u):
        return pltpu.make_async_remote_copy(
            bx.at[half_rows(u), :], bq.at[half_rows(u), :], qsend.at[rem(u, XD)], qrecv.at[u],
            device_id=p_to, device_id_type=MESH,
        )

    def q_direct(u):
        rows = pl.ds(pl.multiple_of(place(far) * KC + rem(u, 2) * HALF, HALF), HALF)
        return pltpu.make_async_remote_copy(
            bx.at[half_rows(u), :], bbuf.at[last_slot, rows, :], qsend.at[rem(u, XD)], qrecv.at[u],
            device_id=p_to, device_id_type=MESH,
        )

    def place(k):
        return jnp.where(k // 2 == y, rem(k, 2), 2 + jnp.where(rem(k, 2) == z, 0, 1))

    def a_loads(s, parts=range(4)):
        slot = rem(s // Q, 2)
        sources = [a_piece(s, 0), a_piece(s, 1), ay.at[s // Q, a_rows(s), :], az.at[s // Q, a_rows(s), :]]
        return [
            pltpu.make_async_copy(
                sources[p], abuf.at[slot, a_rows(s), pl.ds(p * KC, KC)], asem.at[rem(s, AHEAD + Q), p]
            )
            for p in parts
        ]

    def b_loads(t, parts=range(4)):
        slot = rem(t, 2)
        sources = [
            (b_piece(t), i),
            (bp.at[b_rows(t), :], i + swap),
            (bx.at[b_rows(t), :], far),
            (bq.at[b_rows(t), :], far + swap),
        ]
        return [
            pltpu.make_async_copy(
                sources[n][0],
                bbuf.at[slot, pl.ds(pl.multiple_of(place(sources[n][1]) * KC, KC), KC), :],
                bsem.at[slot, n],
            )
            for n in parts
        ]

    def tile(s, n):
        slot, rows, cols = rem(s // Q, 2), a_rows(s), pl.ds(n * tn, tn)
        c_ref[rows, cols] += jnp.dot(
            abuf[slot, rows, :], bbuf[slot, :, cols], preferred_element_type=jnp.float32
        )

    barrier = pltpu.get_barrier_semaphore()
    for to in (z_to, y_to, x_to, p_to):
        pl.semaphore_signal(barrier, inc=1, device_id=to, device_id_type=MESH)
    pl.semaphore_wait(barrier, 4)

    for s in range(YD):
        y_copy(s).start()
    for u in range(XD):
        x_copy(u).start()
    for t in range(PD):
        p_copy(t).start()

    @pl.loop(0, m // 128)
    def _(n):
        rows = pl.ds(pl.multiple_of(n * 128, 128), 128)
        c_ref[rows, :] = jnp.zeros((128, m), jnp.float32)

    def ready(s):
        for ld in a_loads(s):
            ld.wait()

        @pl.when(rem(s, Q) == 0)
        def _():
            for ld in b_loads(s // Q):
                ld.wait()

    def load(s):
        z_copy(s).wait_recv()
        for ld in a_loads(s):
            ld.start()

    def tick(s):
        r, q = s // Q, rem(s, Q)

        @pl.when(s >= ZD)
        def _():
            z_copy(s - ZD).wait_send()

        y_copy(s).wait_recv()

        @pl.when(s < ticks - 2)
        def _():
            z_copy(s).start()

        @pl.when(s == ticks - 2)
        def _():
            pl.semaphore_wait(zfree, 1)
            z_direct(s).start()

        y_copy(s).wait_send()

        @pl.when(s + YD < ticks)
        def _():
            y_copy(s + YD).start()

        @pl.when(s == ticks - 3)
        def _():
            pl.semaphore_wait(yfree, 1)
            w_copy().start()

        @pl.when(rem(q, Q // 2) == Q // 2 - 1)
        def _():
            u = s // (Q // 2)

            @pl.when(u >= XD)
            def _():
                q_copy(u - XD).wait_send()

            x_copy(u).wait_recv()

            @pl.when(u < halves - 2)
            def _():
                q_copy(u).start()

            @pl.when(u == halves - 2)
            def _():
                pl.semaphore_wait(pfree, 1)

            @pl.when(u >= halves - 2)
            def _():
                q_direct(u).start()

            x_copy(u).wait_send()

            @pl.when(u + XD < halves)
            def _():
                x_copy(u + XD).start()

        @pl.when(q == Q - 1)
        def _():
            p_copy(r).wait_send()

            @pl.when(r + PD < rounds)
            def _():
                p_copy(r + PD).start()

        @pl.when(s >= LOAD)
        def _():
            load(s - LOAD)

        @pl.when((q == 0) & (r >= 1))
        def _():
            p_copy(r - 1).wait_recv()
            q_copy(2 * r - 2).wait_recv()
            q_copy(2 * r - 1).wait_recv()
            for ld in b_loads(r - 1):
                ld.start()

    @pl.loop(0, ticks - Q + 1)
    def _(s):
        tick(s)

        @pl.when(s >= WORK)
        def _():
            ready(s - WORK)
            for n in range(NT):
                tile(s - WORK, n)

        @pl.when(s == ticks - Q)
        def _():
            for free, to in ((yfree, y_to), (zfree, z_to), (pfree, p_to)):
                pl.semaphore_signal(free, inc=1, device_id=to, device_id_type=MESH)

    tiles = [(s, n) for s in range(ticks - 2 * Q, ticks - Q) for n in range(NT)]
    share = -(-len(tiles) // (Q - 1))
    for k in range(Q - 1):
        tick(ticks - Q + 1 + k)
        if k == 0:
            p_copy(rounds - 1).wait_recv()
            for ld in b_loads(rounds - 1, range(2)):
                ld.start()
        if k == Q - 2:
            load(ticks - 4)
            for s in range(ticks - 3, ticks):
                for ld in a_loads(s, range(3)):
                    ld.start()
            b_loads(rounds - 1, [2])[0].start()
        for s, n in tiles[k * share : (k + 1) * share]:
            if n == 0:
                ready(s)
            tile(s, n)

    z_copy(ticks - 3).wait_recv()
    a_loads(ticks - 3, [3])[0].start()
    for s in range(ticks - ZD, ticks - 1):
        z_copy(s).wait_send()
    w_copy().wait_send()
    for u in range(halves - XD, halves):
        q_copy(u).wait_send()
    for s in range(ticks - Q, ticks - 2):
        for ld in a_loads(s):
            ld.wait()
    for s in range(ticks - 2, ticks):
        for ld in a_loads(s, range(3)):
            ld.wait()
    for ld in b_loads(rounds - 1, range(3)):
        ld.wait()
    for u in range(halves - 2, halves):
        q_copy(u).wait_recv()
    for s in range(ticks - 2, ticks):
        z_copy(s).wait_recv()


def finish_kernel(slot, c_ref, abuf, bbuf, out, total, sem):
    m = c_ref.shape[0]
    tm, tn = m // Q, m // NT
    ends = [tm // 4, tm // 4, tm // 2]
    writes, top = [], 0
    for k, height in enumerate(ends + [tm] * (Q - 2) + ends[::-1]):
        rows = pl.ds(top, height)
        top += height
        for n in range(NT):
            cols = pl.ds(n * tn, tn)
            total[rows, cols] = c_ref[rows, cols] + jnp.dot(
                abuf[slot, rows, :], bbuf[slot, :, cols], preferred_element_type=jnp.float32
            )
            writes.append(pltpu.make_async_copy(total.at[rows, cols], out.at[rows, cols], sem.at[k, n]))
            writes[-1].start()
    for write in writes:
        write.wait()


def solution(mesh):
    def local_product(a_blk, b_blk):
        m = a_blk.shape[0]
        rounds = m // KC
        ticks = rounds * Q
        any_spec = pl.BlockSpec(memory_space=pl.ANY)
        vmem_spec = pl.BlockSpec(memory_space=pltpu.VMEM)
        dma = pltpu.SemaphoreType.DMA
        c, abuf, bbuf, *_ = pl.pallas_call(
            gather_kernel,
            name="gather",
            out_shape=(
                pltpu.VMEM((m, m), jnp.float32),
                pltpu.VMEM((2, m, 4 * KC), jnp.bfloat16),
                pltpu.VMEM((2, 4 * KC, m), jnp.bfloat16),
                pltpu.HBM((rounds, m, KC), jnp.bfloat16),
                pltpu.HBM((rounds, m, KC), jnp.bfloat16),
                pltpu.HBM((m, m), jnp.bfloat16),
                pltpu.HBM((m, m), jnp.bfloat16),
                pltpu.HBM((m, m), jnp.bfloat16),
            ),
            in_specs=[any_spec] * 2,
            out_specs=(vmem_spec,) * 3 + (any_spec,) * 5,
            scratch_shapes=[
                dma((YD,)), dma((ticks,)), dma((ZD,)), dma((ticks,)), dma, dma((XD,)), dma((2 * rounds,)),
                dma((PD,)), dma((rounds,)), dma((XD,)), dma((2 * rounds,)), dma((AHEAD + Q, 4)), dma((2, 4)),
                *[pltpu.SemaphoreType.REGULAR] * 3,
            ],
            compiler_params=pltpu.CompilerParams(
                collective_id=0, has_side_effects=True, vmem_limit_bytes=4 * 2**20
            ),
        )(a_blk, b_blk)
        c, abuf, bbuf = (pltpu.with_memory_space_constraint(v, pltpu.VMEM) for v in (c, abuf, bbuf))
        return pl.pallas_call(
            functools.partial(finish_kernel, (rounds - 1) % 2),
            name="finish",
            out_shape=(jax.ShapeDtypeStruct((m, m), jnp.float32), pltpu.VMEM((m, m), jnp.float32)),
            in_specs=[vmem_spec] * 3,
            out_specs=(any_spec, vmem_spec),
            input_output_aliases={0: 1},
            scratch_shapes=[dma((Q + 4, NT))],
            compiler_params=pltpu.CompilerParams(vmem_limit_bytes=4 * 2**20),
        )(c, abuf, bbuf)[0]

    return jax.shard_map(
        local_product, mesh=mesh, in_specs=(P("row", "col"), P("row", "col")), out_specs=P("row", ("col", "dep")), check_vma=False
    )
```

```python
import functools

import jax
import jax.numpy as jnp
from jax import lax
from jax.experimental import pallas as pl
from jax.experimental.pallas import tpu as pltpu
from jax.sharding import PartitionSpec as P

MESH = pl.DeviceIdType.MESH
KC = 128
Q = 6
NT = 3
YD = 6
ZD = 6
HALF = KC // 2
XD = 4
PD = 2
LOAD = 4
AHEAD = 3
WORK = Q + 1


def rem(a, b):
    return a % b if isinstance(a, int) else lax.rem(a, b)


def gather_kernel(
    a_ref, b_ref,
    c_ref, abuf, bbuf, ay, az, bx, bp, bq,
    ysend, yrecv, zsend, zrecv, wsend, xsend, xrecv, psend, precv, qsend, qrecv, asem, bsem, yfree, zfree, pfree,
):
    z, y, i = lax.axis_index("dep"), lax.axis_index("col"), lax.axis_index("row")
    m = a_ref.shape[0]
    mq, tn = m // Q, m // NT
    rounds = m // KC
    ticks, halves = rounds * Q, 2 * rounds
    last_slot = (rounds - 1) % 2
    z_to, y_to = {"dep": 1 - z}, {"col": 1 - y}
    swap = 1 - 2 * rem(i, 2)
    far = rem(i + 2, 4)
    x_to, p_to = {"row": far}, {"row": i + swap}

    def a_rows(s):
        return pl.ds(pl.multiple_of(rem(s, Q) * mq, mq), mq)

    def a_piece(s, h):
        return a_ref.at[a_rows(s), pl.ds(pl.multiple_of(h * m + s // Q * KC, KC), KC)]

    def b_rows(t):
        return pl.ds(pl.multiple_of(t * KC, KC), KC)

    def b_piece(t):
        return b_ref.at[b_rows(t), pl.ds(pl.multiple_of(z * m, m), m)]

    def y_copy(s):
        return pltpu.make_async_remote_copy(
            a_piece(s, z), ay.at[s // Q, a_rows(s), :], ysend.at[rem(s, YD)], yrecv.at[s],
            device_id=y_to, device_id_type=MESH,
        )

    def z_copy(s):
        return pltpu.make_async_remote_copy(
            ay.at[s // Q, a_rows(s), :], az.at[s // Q, a_rows(s), :], zsend.at[rem(s, ZD)], zrecv.at[s],
            device_id=z_to, device_id_type=MESH,
        )

    def z_direct(s):
        return pltpu.make_async_remote_copy(
            ay.at[s // Q, a_rows(s), :], abuf.at[last_slot, a_rows(s), pl.ds(3 * KC, KC)],
            zsend.at[rem(s, ZD)], zrecv.at[s],
            device_id=z_to, device_id_type=MESH,
        )

    def w_copy():
        s = ticks - 1
        return pltpu.make_async_remote_copy(
            a_piece(s, 1 - z), abuf.at[last_slot, a_rows(s), pl.ds(3 * KC, KC)], wsend, zrecv.at[s],
            device_id=y_to, device_id_type=MESH,
        )

    def half_rows(u):
        return pl.ds(pl.multiple_of(u * HALF, HALF), HALF)

    def x_copy(u):
        return pltpu.make_async_remote_copy(
            b_ref.at[half_rows(u), pl.ds(pl.multiple_of(z * m, m), m)], bx.at[half_rows(u), :],
            xsend.at[rem(u, XD)], xrecv.at[u],
            device_id=x_to, device_id_type=MESH,
        )

    def p_copy(t):
        return pltpu.make_async_remote_copy(
            b_piece(t), bp.at[b_rows(t), :], psend.at[rem(t, PD)], precv.at[t],
            device_id=p_to, device_id_type=MESH,
        )

    def q_copy(u):
        return pltpu.make_async_remote_copy(
            bx.at[half_rows(u), :], bq.at[half_rows(u), :], qsend.at[rem(u, XD)], qrecv.at[u],
            device_id=p_to, device_id_type=MESH,
        )

    def q_direct(u):
        rows = pl.ds(pl.multiple_of(place(far) * KC + rem(u, 2) * HALF, HALF), HALF)
        return pltpu.make_async_remote_copy(
            bx.at[half_rows(u), :], bbuf.at[last_slot, rows, :], qsend.at[rem(u, XD)], qrecv.at[u],
            device_id=p_to, device_id_type=MESH,
        )

    def place(k):
        return jnp.where(k // 2 == y, rem(k, 2), 2 + jnp.where(rem(k, 2) == z, 0, 1))

    def a_loads(s, parts=range(4)):
        slot = rem(s // Q, 2)
        sources = [a_piece(s, 0), a_piece(s, 1), ay.at[s // Q, a_rows(s), :], az.at[s // Q, a_rows(s), :]]
        return [
            pltpu.make_async_copy(
                sources[p], abuf.at[slot, a_rows(s), pl.ds(p * KC, KC)], asem.at[rem(s, AHEAD + Q), p]
            )
            for p in parts
        ]

    def b_loads(t, parts=range(4)):
        slot = rem(t, 2)
        sources = [
            (b_piece(t), i),
            (bp.at[b_rows(t), :], i + swap),
            (bx.at[b_rows(t), :], far),
            (bq.at[b_rows(t), :], far + swap),
        ]
        return [
            pltpu.make_async_copy(
                sources[n][0],
                bbuf.at[slot, pl.ds(pl.multiple_of(place(sources[n][1]) * KC, KC), KC), :],
                bsem.at[slot, n],
            )
            for n in parts
        ]

    def tile(s, n):
        slot, rows, cols = rem(s // Q, 2), a_rows(s), pl.ds(n * tn, tn)
        c_ref[rows, cols] += jnp.dot(
            abuf[slot, rows, :], bbuf[slot, :, cols], preferred_element_type=jnp.float32
        )

    barrier = pltpu.get_barrier_semaphore()
    for to in (z_to, y_to, x_to, p_to):
        pl.semaphore_signal(barrier, inc=1, device_id=to, device_id_type=MESH)
    pl.semaphore_wait(barrier, 4)

    for s in range(YD):
        y_copy(s).start()
    for u in range(XD):
        x_copy(u).start()
    for t in range(PD):
        p_copy(t).start()

    @pl.loop(0, m // 128)
    def _(n):
        rows = pl.ds(pl.multiple_of(n * 128, 128), 128)
        c_ref[rows, :] = jnp.zeros((128, m), jnp.float32)

    def ready(s):
        for ld in a_loads(s):
            ld.wait()

        @pl.when(rem(s, Q) == 0)
        def _():
            for ld in b_loads(s // Q):
                ld.wait()

    def load(s):
        z_copy(s).wait_recv()
        for ld in a_loads(s):
            ld.start()

    def tick(s):
        r, q = s // Q, rem(s, Q)

        @pl.when(s >= ZD)
        def _():
            z_copy(s - ZD).wait_send()

        y_copy(s).wait_recv()

        @pl.when(s < ticks - 2)
        def _():
            z_copy(s).start()

        @pl.when(s == ticks - 2)
        def _():
            pl.semaphore_wait(zfree, 1)
            z_direct(s).start()

        y_copy(s).wait_send()

        @pl.when(s + YD < ticks)
        def _():
            y_copy(s + YD).start()

        @pl.when(s == ticks - 3)
        def _():
            pl.semaphore_wait(yfree, 1)
            w_copy().start()

        @pl.when(rem(q, Q // 2) == Q // 2 - 1)
        def _():
            u = s // (Q // 2)

            @pl.when(u >= XD)
            def _():
                q_copy(u - XD).wait_send()

            x_copy(u).wait_recv()

            @pl.when(u < halves - 2)
            def _():
                q_copy(u).start()

            @pl.when(u == halves - 2)
            def _():
                pl.semaphore_wait(pfree, 1)

            @pl.when(u >= halves - 2)
            def _():
                q_direct(u).start()

            x_copy(u).wait_send()

            @pl.when(u + XD < halves)
            def _():
                x_copy(u + XD).start()

        @pl.when(q == Q - 1)
        def _():
            p_copy(r).wait_send()

            @pl.when(r + PD < rounds)
            def _():
                p_copy(r + PD).start()

        @pl.when(s >= LOAD)
        def _():
            load(s - LOAD)

        @pl.when((q == 0) & (r >= 1))
        def _():
            p_copy(r - 1).wait_recv()
            q_copy(2 * r - 2).wait_recv()
            q_copy(2 * r - 1).wait_recv()
            for ld in b_loads(r - 1):
                ld.start()

    @pl.loop(0, ticks - Q + 1)
    def _(s):
        tick(s)

        @pl.when(s >= WORK)
        def _():
            ready(s - WORK)
            for n in range(NT):
                tile(s - WORK, n)

        @pl.when(s == ticks - Q)
        def _():
            for free, to in ((yfree, y_to), (zfree, z_to), (pfree, p_to)):
                pl.semaphore_signal(free, inc=1, device_id=to, device_id_type=MESH)

    tiles = [(s, n) for s in range(ticks - 2 * Q, ticks - Q) for n in range(NT)]
    share = -(-len(tiles) // (Q - 1))
    for k in range(Q - 1):
        tick(ticks - Q + 1 + k)
        if k == 0:
            p_copy(rounds - 1).wait_recv()
            for ld in b_loads(rounds - 1, range(2)):
                ld.start()
        if k == Q - 2:
            load(ticks - 4)
            for s in range(ticks - 3, ticks):
                for ld in a_loads(s, range(3)):
                    ld.start()
            b_loads(rounds - 1, [2])[0].start()
        for s, n in tiles[k * share : (k + 1) * share]:
            if n == 0:
                ready(s)
            tile(s, n)

    z_copy(ticks - 3).wait_recv()
    a_loads(ticks - 3, [3])[0].start()
    for s in range(ticks - ZD, ticks - 1):
        z_copy(s).wait_send()
    w_copy().wait_send()
    for u in range(halves - XD, halves):
        q_copy(u).wait_send()
    for s in range(ticks - Q, ticks - 2):
        for ld in a_loads(s):
            ld.wait()
    for s in range(ticks - 2, ticks):
        for ld in a_loads(s, range(3)):
            ld.wait()
    for ld in b_loads(rounds - 1, range(3)):
        ld.wait()
    for u in range(halves - 2, halves):
        q_copy(u).wait_recv()
    for s in range(ticks - 2, ticks):
        z_copy(s).wait_recv()


def finish_kernel(slot, c_ref, abuf, bbuf, out, total, sem):
    m = c_ref.shape[0]
    tm, tn = m // Q, m // NT
    writes = []
    for k in range(Q):
        rows = pl.ds(k * tm, tm)
        for n in range(NT):
            cols = pl.ds(n * tn, tn)
            total[rows, cols] = c_ref[rows, cols] + jnp.dot(
                abuf[slot, rows, :], bbuf[slot, :, cols], preferred_element_type=jnp.float32
            )
            writes.append(pltpu.make_async_copy(total.at[rows, cols], out.at[rows, cols], sem.at[k, n]))
            writes[-1].start()
    for write in writes:
        write.wait()


def solution(mesh):
    def local_product(a_blk, b_blk):
        m = a_blk.shape[0]
        rounds = m // KC
        ticks = rounds * Q
        any_spec = pl.BlockSpec(memory_space=pl.ANY)
        vmem_spec = pl.BlockSpec(memory_space=pltpu.VMEM)
        dma = pltpu.SemaphoreType.DMA
        c, abuf, bbuf, *_ = pl.pallas_call(
            gather_kernel,
            name="gather",
            out_shape=(
                pltpu.VMEM((m, m), jnp.float32),
                pltpu.VMEM((2, m, 4 * KC), jnp.bfloat16),
                pltpu.VMEM((2, 4 * KC, m), jnp.bfloat16),
                pltpu.HBM((rounds, m, KC), jnp.bfloat16),
                pltpu.HBM((rounds, m, KC), jnp.bfloat16),
                pltpu.HBM((m, m), jnp.bfloat16),
                pltpu.HBM((m, m), jnp.bfloat16),
                pltpu.HBM((m, m), jnp.bfloat16),
            ),
            in_specs=[any_spec] * 2,
            out_specs=(vmem_spec,) * 3 + (any_spec,) * 5,
            scratch_shapes=[
                dma((YD,)), dma((ticks,)), dma((ZD,)), dma((ticks,)), dma, dma((XD,)), dma((2 * rounds,)),
                dma((PD,)), dma((rounds,)), dma((XD,)), dma((2 * rounds,)), dma((AHEAD + Q, 4)), dma((2, 4)),
                *[pltpu.SemaphoreType.REGULAR] * 3,
            ],
            compiler_params=pltpu.CompilerParams(
                collective_id=0, has_side_effects=True, vmem_limit_bytes=4 * 2**20
            ),
        )(a_blk, b_blk)
        c, abuf, bbuf = (pltpu.with_memory_space_constraint(v, pltpu.VMEM) for v in (c, abuf, bbuf))
        return pl.pallas_call(
            functools.partial(finish_kernel, (rounds - 1) % 2),
            name="finish",
            out_shape=(jax.ShapeDtypeStruct((m, m), jnp.float32), pltpu.VMEM((m, m), jnp.float32)),
            in_specs=[vmem_spec] * 3,
            out_specs=(any_spec, vmem_spec),
            input_output_aliases={0: 1},
            scratch_shapes=[dma((Q, NT))],
            compiler_params=pltpu.CompilerParams(vmem_limit_bytes=4 * 2**20),
        )(c, abuf, bbuf)[0]

    return jax.shard_map(
        local_product, mesh=mesh, in_specs=(P("row", "col"), P("row", "col")), out_specs=P("row", ("col", "dep")), check_vma=False
    )
```
